512 devices in a mesh: gx: 32 (over y, x_hi, core), gy: 16 (over x_lo, z).
Axes of the slice: x: 4 (x_hi: 2, x_lo: 2; x = x_hi * 2 + x_lo), y: 8, z: 8, core: 2. Of those that a mesh axis runs over, the one named last changes fastest.
Arguments:
- prior_fields: bfloat16 [512, 64, 4096], P('gx', 'gy'), may hold values from -17 to 17
- measured_spread: bfloat16 [512, 16, 4096], P(None, 'gy', 'gx'), may hold values from -10 to 10
- scaled_misfit: bfloat16 [16, 4096], P('gy', 'gx'), may hold values from -12 to 12
- sensor_line_inside: int32 [16, 4096], P('gy', 'gx'), may hold values from 0 to 3
Outputs:
- analysis: bfloat16 [512, 64, 4096], P(None, 'gy', 'gx')
The draws below stay inside these ranges and needn't reach their ends.
All inputs are finite; a program needn't handle non-finite values. Where the reference program divides by a largest or mean magnitude, that divisor is 1e-20 or more.
Results may differ from the reference program's by a relative error of at most 0.0053.
Values may be sent and summed in bfloat16 or wider, within the bound.
A program may use at most 64 MiB of HBM per device.

```python
import jax
import jax.numpy as jnp
from jax import lax

K = 512
BLOCK_WIDTH_X = 128
CY = 4
OY = 1
OX = 128
CP = 2
NEWTON = 2
NY = 64
NX = 4096
NOY = 16
NOX = 4096
N_GX = 32
N_GY = 16


def member_loadings(base_key, mode_count):
    sign_key, size_key = jax.random.split(jax.random.fold_in(base_key, 101))
    sign_values = jax.random.rademacher(sign_key, (K, mode_count), dtype=jnp.float32)
    magnitude = jax.random.uniform(size_key, (K, mode_count), jnp.float32, 0.6, 1.4)
    return sign_values * magnitude


def mode_sum(base_key, salt_value, cell_count, leading, slope, noise_scale, limit_value, levels):
    mode_count = max(4, K // 4)
    loadings = member_loadings(base_key, mode_count)
    field_key, noise_key = jax.random.split(jax.random.fold_in(base_key, salt_value))
    mode_order = jnp.arange(1, mode_count + 1, dtype=jnp.float32)
    strengths = leading * mode_order ** (-slope)
    fields = jax.random.truncated_normal(field_key, -4.0, 4.0, (mode_count, cell_count), jnp.float32)
    noise_part = noise_scale * jax.random.truncated_normal(noise_key, -4.0, 4.0, (K, cell_count), jnp.float32)
    mode_part = jnp.dot(loadings * strengths[None, :], fields, precision=lax.Precision.HIGHEST)
    return jnp.clip((mode_part + noise_part) * levels[None, :], -limit_value, limit_value)


def draw_prior_fields(key, part):
    cell_count = NY * NX
    levels = jnp.ones((cell_count,), jnp.float32)
    member_part = mode_sum(key, 202, cell_count, 1.0, 0.5, 0.5, 16.0, levels)
    mean_key = jax.random.fold_in(key, 303)
    mean_field = 0.2 * jax.random.truncated_normal(mean_key, -4.0, 4.0, (cell_count,), jnp.float32)
    return (member_part + mean_field[None, :]).reshape(K, NY, NX).astype(jnp.bfloat16)


def draw_measured_spread(key, part):
    cell_count = NOY * NOX
    level_key = jax.random.fold_in(key, 505)
    tile_levels = jnp.exp(jax.random.uniform(level_key, (NOY, NOX // OX), jnp.float32, -1.2, 1.2))
    levels = jnp.repeat(tile_levels, OX, axis=1).reshape(-1)
    return mode_sum(key, 404, cell_count, 0.045, 0.15, 0.3, 10.0, levels).reshape(K, NOY, NOX).astype(jnp.bfloat16)


def touch_ends(array, stream_key, low, high):
    longest = array.shape.index(max(array.shape))
    spots = []
    for shift in (0, 1):
        where = [jax.random.randint(jax.random.fold_in(stream_key, axis), (), 0, length) for axis, length in enumerate(array.shape)]
        where[longest] = (where[longest] + shift) % array.shape[longest]
        spots.append(tuple(where))
    return array.at[spots[0]].set(low).at[spots[1]].set(high)


def block_levels(own_key, dims, cuts, low, high):
    factor_of = 1.0
    for dim, shards_of in cuts:
        heights = jax.random.uniform(jax.random.fold_in(jax.random.fold_in(own_key, 6), dim), (shards_of,), jnp.float32, low / len(cuts), high / len(cuts))
        factor_of = factor_of * jnp.repeat(jnp.exp(heights), dims[dim] // shards_of).reshape((-1,) + (1,) * (len(dims) - 1 - dim))
    return factor_of


def gaussian(stream_key, extent, scale, bound, cuts=(), kind=jnp.bfloat16):
    values = scale * jax.random.normal(stream_key, extent, jnp.float32)
    if cuts:
        values = values * block_levels(stream_key, extent, cuts, -0.22, 0.18)
    return jnp.clip(values, -bound, bound).astype(kind)


def setup_inputs(seed: int = 0) -> dict:
    splits = jax.random.split(jax.random.key(seed), 5)
    return {
        "prior_fields": draw_prior_fields(jax.random.fold_in(splits[4], 71), 0),
        "measured_spread": draw_measured_spread(jax.random.fold_in(splits[4], 71), 0),
        "scaled_misfit": gaussian(splits[2], (NOY, NOX), 2.0, 12.0, ((0, 16), (1, 32))),
        "sensor_line_inside": touch_ends(jax.random.randint(splits[3], (NOY, NOX), 0, CY), jax.random.fold_in(splits[3], 1), 0, CY - 1).astype(jnp.int32),
    }


highest = lax.Precision.HIGHEST

def localize(positions, centre, radius):
    distance = (positions - centre) / radius
    return jnp.exp(-0.5 * distance * distance)

def newton_weights(gram_matrix, drive_vector, sweeps):
    sample_count = gram_matrix.shape[0]
    identity = jnp.eye(sample_count, dtype=jnp.float32)
    scaled_gram = identity + gram_matrix / (sample_count - 1.0)
    row_bound = jnp.max(lax.optimization_barrier(jnp.sum(jnp.abs(scaled_gram), axis=1)))
    iterate = scaled_gram / row_bound
    inverse = identity
    for newton_step in range(sweeps):
        if newton_step == 0:
            factor = 0.5 * (3.0 * identity - iterate)
            inverse = factor
        else:
            factor = 0.5 * (3.0 * identity - jnp.dot(inverse, iterate, precision=highest))
            inverse = jnp.dot(factor, inverse, precision=highest)
        if newton_step + 1 < sweeps:
            iterate = jnp.dot(iterate, factor, precision=highest)
    first_pass = jnp.dot(inverse, drive_vector, precision=highest)
    mean_weights = jnp.dot(inverse, first_pass, precision=highest) / (row_bound * (sample_count - 1.0))
    return (inverse / jnp.sqrt(row_bound) + mean_weights[:, None]).astype(jnp.bfloat16)

def coarse_weights(obs_block, innov_block, positions, centre, radius):
    locality = localize(positions, centre, radius)
    scaled = (obs_block.astype(jnp.float32) * locality[None, :]).astype(jnp.bfloat16)
    gram_matrix = lax.dot_general(scaled, obs_block, (((1,), (1,)), ((), ())), preferred_element_type=jnp.float32)
    drive_vector = jnp.dot(scaled, innov_block, preferred_element_type=jnp.float32)
    return newton_weights(gram_matrix, drive_vector, NEWTON)

def hat_weights(row_centres, centre, spacing, height):
    clipped = jnp.clip(row_centres, 0.5 * spacing, height - 0.5 * spacing)
    return jnp.maximum(0.0, 1.0 - jnp.abs(clipped - centre) / spacing)

def apply_weights(transform, state_block, interp):
    sample_count, row_count, cell_count = state_block.shape
    product = lax.dot_general(transform, state_block.reshape(sample_count, row_count * cell_count), (((0,), (0,)), ((), ())), preferred_element_type=jnp.float32)
    return product.reshape(sample_count, row_count, cell_count) * interp[None, :, None]

def reference(prior_fields, measured_spread, scaled_misfit, sensor_line_inside):
    sample_count = prior_fields.shape[0]
    spacing = CY // CP
    point_count = CP * N_GY
    window = 2 * spacing
    pert_tiles = jnp.pad(measured_spread.reshape(sample_count, N_GY, OY, N_GX, OX), ((0, 0), (1, 1), (0, 0), (0, 0), (0, 0)))
    innov_tiles = jnp.pad(scaled_misfit.reshape(N_GY, OY, N_GX, OX), ((1, 1), (0, 0), (0, 0), (0, 0)))
    row_tiles = jnp.pad(sensor_line_inside.reshape(N_GY, OY, N_GX, OX), ((1, 1), (0, 0), (0, 0), (0, 0)))
    tile_base = (jnp.arange(N_GY + 2, dtype=jnp.int32) - 1) * CY
    pos_tiles = (tile_base[:, None, None, None] + row_tiles).astype(jnp.float32) + 0.5

    def one_column(block_for_lane):
        pert_column = lax.dynamic_index_in_dim(pert_tiles, block_for_lane, 3, keepdims=False)
        innov_column = lax.dynamic_index_in_dim(innov_tiles, block_for_lane, 2, keepdims=False)
        pos_column = lax.dynamic_index_in_dim(pos_tiles, block_for_lane, 2, keepdims=False)

        def one_point(point_index):
            row_tile = point_index // CP
            obs_block = lax.dynamic_slice_in_dim(pert_column, row_tile, 3, 1).reshape(sample_count, -1)
            innov_block = lax.dynamic_slice_in_dim(innov_column, row_tile, 3, 0).reshape(-1)
            positions = lax.dynamic_slice_in_dim(pos_column, row_tile, 3, 0).reshape(-1)
            centre = (point_index.astype(jnp.float32) + 0.5) * spacing
            return coarse_weights(obs_block, innov_block, positions, centre, float(CY))
        all_weights = lax.map(one_point, jnp.arange(point_count, dtype=jnp.int32))
        prior_by_lane = lax.dynamic_slice_in_dim(prior_fields, block_for_lane * BLOCK_WIDTH_X, BLOCK_WIDTH_X, 2)
        state_mean = lax.optimization_barrier(jnp.sum(prior_by_lane, axis=0, dtype=jnp.float32)) / sample_count
        deviation = (prior_by_lane.astype(jnp.float32) - state_mean[None]).astype(jnp.bfloat16)

        def add_point(increment, point_index):
            first_row = jnp.clip(point_index * spacing - spacing // 2, 0, NY - window)
            state_block = lax.dynamic_slice_in_dim(deviation, first_row, window, 1)
            row_centres = (first_row + jnp.arange(window, dtype=jnp.int32)).astype(jnp.float32) + 0.5
            centre = (point_index.astype(jnp.float32) + 0.5) * spacing
            interp = hat_weights(row_centres, centre, spacing, NY)
            term_block = apply_weights(all_weights[point_index], state_block, interp)
            current = lax.dynamic_slice_in_dim(increment, first_row, window, 1)
            return (lax.dynamic_update_slice_in_dim(increment, current + term_block, first_row, 1), None)
        increment, unused = lax.scan(add_point, jnp.zeros(deviation.shape, jnp.float32), jnp.arange(point_count, dtype=jnp.int32))
        return (state_mean[None] + increment).astype(jnp.bfloat16)
    columns = lax.map(one_column, jnp.arange(N_GX, dtype=jnp.int32))
    return jnp.transpose(columns, (1, 2, 0, 3)).reshape(sample_count, NY, N_GX * BLOCK_WIDTH_X)
```

```python
import functools

import jax
import jax.numpy as jnp
from jax import lax
from jax.experimental import pallas as pl
from jax.experimental.pallas import tpu as pltpu
from jax.sharding import PartitionSpec as P

MESH = pl.DeviceIdType.MESH
NT = (((1,), (1,)), ((), ()))
NN = (((1,), (0,)), ((), ()))


def mm(a, b, dims=NN):
    return lax.dot_general(a, b, dims, preferred_element_type=jnp.float32)


def halves(x):
    high = x.astype(jnp.bfloat16)
    low = (x - high.astype(jnp.float32)).astype(jnp.bfloat16)
    return high, low


def hat(row, point, spacing, height):
    r = jnp.clip(row.astype(jnp.float32) + 0.5, 0.5 * spacing, height - 0.5 * spacing)
    centre = (point.astype(jnp.float32) + 0.5) * spacing
    return jnp.maximum(0.0, 1.0 - jnp.abs(r - centre) / spacing)


def kernel(
    n_gx,
    n_gy,
    prior_ref,
    spread_ref,
    misfit_ref,
    line_ref,
    out_ref,
    recv,
    obs,
    obs_misfit,
    obs_line,
    transforms,
    mixed,
    wide,
    a2a_send,
    a2a_recv,
    obs_send,
    obs_recv,
    own_sem,
):
    gx = lax.axis_index("gx")
    gy = lax.axis_index("gy")
    own_members, rows, _ = prior_ref.shape
    members, lanes = spread_ref.shape
    spacing = rows // 2
    height = rows * n_gy
    offsets = (1, -1, 2, -2)

    def to_row(step):
        return lax.rem(gy + step + n_gy, n_gy)

    def peer(step):
        return lax.rem(gx + step, n_gx)

    barrier = pltpu.get_barrier_semaphore()

    def greet(step, carry):
        pl.semaphore_signal(barrier, inc=1, device_id={"gx": peer(step)}, device_id_type=MESH)
        return carry

    for step in offsets:
        pl.semaphore_signal(barrier, inc=1, device_id={"gy": to_row(step)}, device_id_type=MESH)
    lax.fori_loop(1, n_gx, greet, 0)

    own_piece = pltpu.make_async_copy(
        prior_ref.at[:, :, pl.ds(pl.multiple_of(gx * lanes, lanes), lanes)],
        recv.at[pl.ds(gx * own_members, own_members)],
        own_sem.at[0],
    )
    own_obs = pltpu.make_async_copy(spread_ref, obs.at[pl.ds(0, members), pl.ds(2 * lanes, lanes)], own_sem.at[1])
    own_misfit = pltpu.make_async_copy(misfit_ref, obs_misfit.at[2], own_sem.at[2])
    own_line = pltpu.make_async_copy(line_ref, obs_line.at[2], own_sem.at[3])
    own_piece.start()
    own_obs.start()
    own_misfit.start()
    own_line.start()

    pl.semaphore_wait(barrier, n_gx - 1 + len(offsets))

    def obs_copies(k):
        step = offsets[k]
        slot = 2 - step
        ends = (
            (spread_ref, obs.at[pl.ds(0, members), pl.ds(slot * lanes, lanes)]),
            (misfit_ref, obs_misfit.at[slot]),
            (line_ref, obs_line.at[slot]),
        )
        return [
            pltpu.make_async_remote_copy(
                src_ref=src,
                dst_ref=dst,
                send_sem=obs_send.at[k, j],
                recv_sem=obs_recv.at[k, j],
                device_id={"gy": to_row(step)},
                device_id_type=MESH,
            )
            for j, (src, dst) in enumerate(ends)
        ]

    def piece(step):
        there = peer(step)
        return pltpu.make_async_remote_copy(
            src_ref=prior_ref.at[:, :, pl.ds(pl.multiple_of(there * lanes, lanes), lanes)],
            dst_ref=recv.at[pl.ds(gx * own_members, own_members)],
            send_sem=a2a_send.at[step],
            recv_sem=a2a_recv.at[step],
            device_id={"gx": there},
            device_id_type=MESH,
        )

    sends = [obs_copies(k) for k in range(len(offsets))]
    for k in (0, 1):
        for copy in sends[k]:
            copy.start()

    def send(step, carry):
        piece(step).start()
        return carry

    lax.fori_loop(1, n_gx, send, 0)
    for k in (2, 3):
        for copy in sends[k]:
            copy.start()

    own_obs.wait()
    own_misfit.wait()
    own_line.wait()

    def arrived(k):
        for copy in sends[k]:
            copy.wait_recv()

    arrived(0)
    arrived(1)

    def point_transform(i, carry):
        @pl.when(i == 2)
        def _():
            arrived(2)
            arrived(3)

        which = jnp.where(i == 2, -1, jnp.where(i == 3, 2, i))
        first = jnp.where(i == 2, 0, jnp.where(i == 3, 2, 1))
        point = 2 * gy + which
        centre = (point.astype(jnp.float32) + 0.5) * spacing
        local = []
        values = []
        for s in range(3):
            tile = gy + first + s - 2
            line = obs_line[first + s].astype(jnp.float32)
            position = (tile * rows).astype(jnp.float32) + line + 0.5
            distance = (position - centre) / float(rows)
            there = jnp.where(jnp.logical_and(tile >= 0, tile < n_gy), 1.0, 0.0)
            local.append(jnp.exp(-0.5 * distance * distance) * there)
            values.append(obs_misfit[first + s])
        locality = jnp.concatenate(local, axis=1)
        misfit = jnp.concatenate(values, axis=1)
        block = obs[:, pl.ds(pl.multiple_of(first * lanes, lanes), 3 * lanes)]
        scaled = (block.astype(jnp.float32) * locality).astype(jnp.bfloat16)
        gram = mm(block, scaled, NT)
        drive = mm(jnp.broadcast_to(misfit, (16, 3 * lanes)), scaled, NT)[:8]

        eye = jnp.where(
            lax.broadcasted_iota(jnp.int32, (members, members), 0)
            == lax.broadcasted_iota(jnp.int32, (members, members), 1),
            1.0,
            0.0,
        )
        m = eye + gram * (1.0 / (members - 1.0))
        sums = jnp.sum(jnp.abs(m), axis=0, keepdims=True)
        bound = jnp.max(sums, axis=1, keepdims=True)
        y = m * (1.0 / bound)
        yh, yl = halves(y)
        q = mm(yh, yh) + (mm(yh, yl) + mm(yl, yh))
        qh, ql = halves(q)
        r = 0.0625 * q - 0.5625 * y
        rh, rl = halves(r)
        z = 2.25 * eye - 2.4375 * y + 1.6875 * q + (mm(qh, rh) + (mm(qh, rl) + mm(ql, rh)))
        zh, zl = halves(z)

        def through(v):
            vh, vl = halves(v)
            both = jnp.concatenate([vh, vl], axis=0)
            p = mm(both, zh)
            return p[:8] + p[8:] + mm(both, zl)[:8]

        weights = through(through(drive))[:1] * (1.0 / (bound * (members - 1.0)))
        transforms[i] = z * lax.rsqrt(bound) + weights
        return carry

    lax.fori_loop(0, 4, point_transform, 0)

    pairs = ((0, -1), (0, 1), (0, 1), (1, 2))
    place = {0: 0, 1: 1, -1: 2, 2: 3}
    for row, (p, q) in enumerate(pairs):
        at = gy * rows + row
        wp = hat(at, 2 * gy + p, float(spacing), float(height))
        wq = hat(at, 2 * gy + q, float(spacing), float(height))
        mixed[row] = (wp * transforms[place[p]] + wq * transforms[place[q]]).astype(jnp.bfloat16)

    own_piece.wait()

    def land(step, carry):
        piece(step).wait_recv()
        return carry

    lax.fori_loop(1, n_gx, land, 0)

    wide[...] = recv.reshape(members * rows, lanes)[...].astype(jnp.float32)
    for row in range(rows):
        x = wide[pl.ds(row, members, stride=rows), :]
        mean = jnp.sum(x, axis=0, keepdims=True) * (1.0 / members)
        deviation = (x - mean).astype(jnp.bfloat16)
        wide[pl.ds(row, members, stride=rows), :] = mm(mixed[row], deviation) + mean
    out_ref[...] = wide[...].astype(jnp.bfloat16)

    def sent(step, carry):
        piece(step).wait_send()
        return carry

    lax.fori_loop(1, n_gx, sent, 0)
    for copies in sends:
        for copy in copies:
            copy.wait_send()


def solution(mesh):
    n_gx, n_gy = mesh.shape["gx"], mesh.shape["gy"]

    def on_device(prior, spread, misfit, line):
        members, _, lanes = spread.shape
        rows = prior.shape[1]
        out = pl.pallas_call(
            functools.partial(kernel, n_gx, n_gy),
            out_shape=jax.ShapeDtypeStruct((members * rows, lanes), jnp.bfloat16),
            in_specs=[pl.BlockSpec(memory_space=pl.ANY)] * 4,
            out_specs=pl.BlockSpec(memory_space=pltpu.VMEM),
            scratch_shapes=[
                pltpu.VMEM((members, rows, lanes), jnp.bfloat16),
                pltpu.VMEM((members, 5 * lanes), jnp.bfloat16),
                pltpu.VMEM((5, 1, lanes), jnp.bfloat16),
                pltpu.VMEM((5, 1, lanes), jnp.int32),
                pltpu.VMEM((4, members, members), jnp.float32),
                pltpu.VMEM((rows, members, members), jnp.bfloat16),
                pltpu.VMEM((members * rows, lanes), jnp.float32),
                pltpu.SemaphoreType.DMA((n_gx,)),
                pltpu.SemaphoreType.DMA((n_gx,)),
                pltpu.SemaphoreType.DMA((4, 3)),
                pltpu.SemaphoreType.DMA((4, 3)),
                pltpu.SemaphoreType.DMA((4,)),
            ],
            compiler_params=pltpu.CompilerParams(
                collective_id=0, has_side_effects=True, vmem_limit_bytes=48 * 1024 * 1024
            ),
            name="analysis",
        )(prior, spread.reshape(members, lanes), misfit, line)
        return out.reshape(members, rows, lanes)

    return jax.shard_map(
        on_device,
        mesh=mesh,
        in_specs=(P("gx", "gy", None), P(None, "gy", "gx"), P("gy", "gx"), P("gy", "gx")),
        out_specs=P(None, "gy", "gx"),
        check_vma=False,
    )
```

```python
import functools

import jax
import jax.numpy as jnp
from jax import lax
from jax.experimental import pallas as pl
from jax.experimental.pallas import tpu as pltpu
from jax.sharding import PartitionSpec as P

MESH = pl.DeviceIdType.MESH
NT = (((1,), (1,)), ((), ()))
NN = (((1,), (0,)), ((), ()))
OFFSETS = (1, -1, 2, -2)


def mm(a, b, dims=NN):
    return lax.dot_general(a, b, dims, preferred_element_type=jnp.float32)


def halves(x):
    high = x.astype(jnp.bfloat16)
    return high, x - high.astype(jnp.float32)


def hat(row, point, spacing, height):
    r = jnp.clip(row.astype(jnp.float32) + 0.5, 0.5 * spacing, height - 0.5 * spacing)
    centre = (point.astype(jnp.float32) + 0.5) * spacing
    return jnp.maximum(0.0, 1.0 - jnp.abs(r - centre) / spacing)


def kernel(
    n_gx,
    n_gy,
    prior_ref,
    spread_ref,
    misfit_ref,
    line_ref,
    out_ref,
    recv,
    obs,
    obs_misfit,
    obs_line,
    eye,
    inner,
    mixed,
    wide,
    a2a_send,
    a2a_recv,
    obs_send,
    obs_recv,
    own_sem,
    go_sem,
    ack_sem,
):
    gx = lax.axis_index("gx")
    gy = lax.axis_index("gy")
    own_members, rows, _ = prior_ref.shape
    members, lanes = spread_ref.shape
    spacing = rows // 2
    height = rows * n_gy
    split = n_gy // 2
    leader = (n_gx // 8) * 5 - 1
    upper = gy >= split

    def to_row(step):
        return {"gy": gy + step}

    def peer(step):
        return lax.rem(gx + step, n_gx)

    exists = {step: jnp.logical_and(gy + step >= 0, gy + step < n_gy) for step in OFFSETS}
    crosses = {
        step: jnp.logical_and(exists[step], jnp.logical_xor(upper, gy + step >= split)) for step in OFFSETS
    }
    near = {step: jnp.logical_and(exists[step], jnp.logical_not(crosses[step])) for step in OFFSETS}

    def count(flags):
        return sum(flags[step].astype(jnp.int32) for step in OFFSETS)

    barrier = pltpu.get_barrier_semaphore()
    for step in OFFSETS:

        @pl.when(jnp.logical_and(exists[step], jnp.logical_or(upper, jnp.logical_not(crosses[step]))))
        def _():
            pl.semaphore_signal(barrier, inc=1, device_id=to_row(step), device_id_type=MESH)

    own_piece = pltpu.make_async_copy(
        prior_ref.at[:, :, pl.ds(pl.multiple_of(gx * lanes, lanes), lanes)],
        recv.at[pl.ds(gx * own_members, own_members)],
        own_sem.at[0],
    )
    own_obs = pltpu.make_async_copy(spread_ref, obs.at[:, pl.ds(2 * lanes, lanes)], own_sem.at[1])
    own_misfit = pltpu.make_async_copy(misfit_ref, obs_misfit.at[2], own_sem.at[2])
    own_line = pltpu.make_async_copy(line_ref, obs_line.at[2], own_sem.at[3])
    for copy in (own_piece, own_obs, own_misfit, own_line):
        copy.start()

    def obs_copies(k):
        step = OFFSETS[k]
        slot = 2 - step
        ends = (
            (spread_ref, obs.at[:, pl.ds(slot * lanes, lanes)]),
            (misfit_ref, obs_misfit.at[slot]),
            (line_ref, obs_line.at[slot]),
        )
        return [
            pltpu.make_async_remote_copy(
                src_ref=src,
                dst_ref=dst,
                send_sem=obs_send.at[k, j],
                recv_sem=obs_recv.at[k, j],
                device_id=to_row(step),
                device_id_type=MESH,
            )
            for j, (src, dst) in enumerate(ends)
        ]

    sends = [obs_copies(k) for k in range(len(OFFSETS))]

    def start_obs(k, flag):
        @pl.when(flag)
        def _():
            for copy in sends[k]:
                copy.start()

    def piece(step):
        there = peer(step)
        return pltpu.make_async_remote_copy(
            src_ref=prior_ref.at[:, :, pl.ds(pl.multiple_of(there * lanes, lanes), lanes)],
            dst_ref=recv.at[pl.ds(gx * own_members, own_members)],
            send_sem=a2a_send.at[step],
            recv_sem=a2a_recv.at[step],
            device_id={"gx": there},
            device_id_type=MESH,
        )

    expected = jnp.where(upper, count(near), count(exists))
    expected = expected + jnp.where(gx == leader, n_gx - 1, 0)
    pl.semaphore_wait(barrier, expected)

    for k, step in enumerate(OFFSETS):

        @pl.when(jnp.logical_and(crosses[step], jnp.logical_not(upper)))
        def _():
            pl.semaphore_signal(ack_sem, inc=1, device_id=to_row(step), device_id_type=MESH)

    for k, step in enumerate(OFFSETS):
        start_obs(k, jnp.logical_and(exists[step], jnp.logical_or(near[step], jnp.logical_not(upper))))

    @pl.when(gx != leader)
    def _():
        pl.semaphore_signal(barrier, inc=1, device_id={"gx": leader}, device_id_type=MESH)
        pl.semaphore_wait(go_sem, 1)

    @pl.when(gx == leader)
    def _():
        def go(step, carry):
            pl.semaphore_signal(go_sem, inc=1, device_id={"gx": peer(step)}, device_id_type=MESH)
            return carry

        lax.fori_loop(1, n_gx, go, 0)

    def send(t, carry):
        far = n_gx // 2 + ((t + 1) // 2) * (1 - 2 * lax.rem(t, 2))
        piece(far).start()
        return carry

    lax.fori_loop(0, n_gx - 1, send, 0)

    n_cross = count(crosses)

    @pl.when(jnp.logical_and(upper, n_cross > 0))
    def _():
        pl.semaphore_wait(ack_sem, n_cross)
        for k, step in enumerate(OFFSETS):
            start_obs(k, crosses[step])

    eye[...] = jnp.where(
        lax.broadcasted_iota(jnp.int32, (members, members), 0)
        == lax.broadcasted_iota(jnp.int32, (members, members), 1),
        1.0,
        0.0,
    )
    for step in OFFSETS:
        slot = 2 + step

        @pl.when(jnp.logical_not(exists[step]))
        def _():
            obs[:, slot * lanes : (slot + 1) * lanes] = jnp.zeros((members, lanes), jnp.bfloat16)
            obs_misfit[slot] = jnp.zeros((1, lanes), jnp.bfloat16)
            obs_line[slot] = jnp.zeros((1, lanes), jnp.int32)

    own_obs.wait()
    own_misfit.wait()
    own_line.wait()

    def arrived(k):
        @pl.when(exists[-OFFSETS[k]])
        def _():
            for copy in sends[k]:
                copy.wait_recv()

    def transform(which, first):
        point = 2 * gy + which
        centre = (point.astype(jnp.float32) + 0.5) * spacing
        local = []
        for s in range(first, first + 3):
            tile = gy + s - 2
            position = (tile * rows).astype(jnp.float32) + obs_line[s].astype(jnp.float32) + 0.5
            distance = (position - centre) / float(rows)
            there = jnp.where(jnp.logical_and(tile >= 0, tile < n_gy), 1.0, 0.0)
            local.append(jnp.exp(-0.5 * distance * distance) * there)
        locality = jnp.concatenate(local, axis=1)
        misfit = jnp.concatenate([obs_misfit[s] for s in range(first, first + 3)], axis=1)
        block = obs[:, first * lanes : (first + 3) * lanes]
        scaled = (block.astype(jnp.float32) * locality).astype(jnp.bfloat16)
        gram = mm(block, scaled, NT)
        drive = mm(jnp.broadcast_to(misfit, (16, 3 * lanes)), scaled, NT)[:8]

        m = eye[...] + gram * (1.0 / (members - 1.0))
        bound = jnp.max(jnp.sum(jnp.abs(m), axis=0, keepdims=True), axis=1, keepdims=True)
        y = m * (1.0 / bound)
        yh, yl = halves(y)
        q = mm(
            jnp.concatenate([yh, yh], axis=1),
            jnp.concatenate([yh, (yl + yl).astype(jnp.bfloat16)], axis=0),
        )
        r = 0.0625 * q - 0.5625 * y
        z = mm(q.astype(jnp.bfloat16), r.astype(jnp.bfloat16))
        z = 2.25 * eye[...] - 2.4375 * y + 1.6875 * q + z
        zh, zl = halves(z)
        zl = zl.astype(jnp.bfloat16)

        def through(v):
            vh, vl = halves(v)
            both = jnp.concatenate([vh, vl.astype(jnp.bfloat16)], axis=0)
            p = mm(both, zh)
            return p[:8] + p[8:] + mm(both, zl)[:8]

        weights = through(through(drive))[:1] * (1.0 / (bound * (members - 1.0)))
        return z * lax.rsqrt(bound) + weights

    def weight(row, which):
        return hat(gy * rows + row, 2 * gy + which, float(spacing), float(height))

    arrived(0)
    arrived(1)
    t0 = transform(0, 1)
    t1 = transform(1, 1)
    inner[0] = t0
    inner[1] = t1
    mixed[1] = (weight(1, 0) * t0 + weight(1, 1) * t1).astype(jnp.bfloat16)
    mixed[2] = (weight(2, 0) * t0 + weight(2, 1) * t1).astype(jnp.bfloat16)
    arrived(2)
    arrived(3)
    mixed[0] = (weight(0, 0) * inner[0] + weight(0, -1) * transform(-1, 0)).astype(jnp.bfloat16)
    mixed[3] = (weight(3, 1) * inner[1] + weight(3, 2) * transform(2, 2)).astype(jnp.bfloat16)

    own_piece.wait()

    def land(step, carry):
        piece(step).wait_recv()
        return carry

    lax.fori_loop(1, n_gx, land, 0)

    wide[...] = recv.reshape(members * rows, lanes)[...].astype(jnp.float32)
    for row in range(rows):
        x = wide[pl.ds(row, members, stride=rows), :]
        mean = jnp.sum(x, axis=0, keepdims=True) * (1.0 / members)
        deviation = (x - mean).astype(jnp.bfloat16)
        wide[pl.ds(row, members, stride=rows), :] = mm(mixed[row], deviation) + mean
    out_ref[...] = wide[...].astype(jnp.bfloat16)

    def sent(step, carry):
        piece(step).wait_send()
        return carry

    lax.fori_loop(1, n_gx, sent, 0)
    for k, step in enumerate(OFFSETS):

        @pl.when(exists[step])
        def _():
            for copy in sends[k]:
                copy.wait_send()


def solution(mesh):
    n_gx, n_gy = mesh.shape["gx"], mesh.shape["gy"]

    def on_device(prior, spread, misfit, line):
        members, _, lanes = spread.shape
        rows = prior.shape[1]
        out = pl.pallas_call(
            functools.partial(kernel, n_gx, n_gy),
            out_shape=jax.ShapeDtypeStruct((members * rows, lanes), jnp.bfloat16),
            in_specs=[pl.BlockSpec(memory_space=pltpu.HBM)] * 4,
            out_specs=pl.BlockSpec(memory_space=pltpu.VMEM),
            scratch_shapes=[
                pltpu.VMEM((members, rows, lanes), jnp.bfloat16),
                pltpu.VMEM((members, 5 * lanes), jnp.bfloat16),
                pltpu.VMEM((5, 1, lanes), jnp.bfloat16),
                pltpu.VMEM((5, 1, lanes), jnp.int32),
                pltpu.VMEM((members, members), jnp.float32),
                pltpu.VMEM((2, members, members), jnp.float32),
                pltpu.VMEM((rows, members, members), jnp.bfloat16),
                pltpu.VMEM((members * rows, lanes), jnp.float32),
                pltpu.SemaphoreType.DMA((n_gx,)),
                pltpu.SemaphoreType.DMA((n_gx,)),
                pltpu.SemaphoreType.DMA((4, 3)),
                pltpu.SemaphoreType.DMA((4, 3)),
                pltpu.SemaphoreType.DMA((4,)),
                pltpu.SemaphoreType.REGULAR,
                pltpu.SemaphoreType.REGULAR,
            ],
            compiler_params=pltpu.CompilerParams(
                collective_id=0, has_side_effects=True, vmem_limit_bytes=67043328
            ),
            name="analysis",
        )(prior, spread.reshape(members, lanes), misfit, line)
        return out.reshape(members, rows, lanes)

    return jax.shard_map(
        on_device,
        mesh=mesh,
        in_specs=(P("gx", "gy", None), P(None, "gy", "gx"), P("gy", "gx"), P("gy", "gx")),
        out_specs=P(None, "gy", "gx"),
        check_vma=False,
    )
```

```python
import functools

import jax
import jax.numpy as jnp
from jax import lax
from jax.experimental import pallas as pl
from jax.experimental.pallas import tpu as pltpu
from jax.sharding import PartitionSpec as P

MESH = pl.DeviceIdType.MESH
NT = (((1,), (1,)), ((), ()))
NN = (((1,), (0,)), ((), ()))
OFFSETS = (1, -1, 2, -2)


def mm(a, b, dims=NN):
    return lax.dot_general(a, b, dims, preferred_element_type=jnp.float32)


def halves(x):
    high = x.astype(jnp.bfloat16)
    return high, x - high.astype(jnp.float32)


def hat(row, point, spacing, height):
    r = jnp.clip(row.astype(jnp.float32) + 0.5, 0.5 * spacing, height - 0.5 * spacing)
    centre = (point.astype(jnp.float32) + 0.5) * spacing
    return jnp.maximum(0.0, 1.0 - jnp.abs(r - centre) / spacing)


def kernel(
    n_gx,
    n_gy,
    prior_ref,
    spread_ref,
    misfit_ref,
    line_ref,
    out_ref,
    recv,
    obs,
    obs_misfit,
    obs_line,
    inner,
    mixed,
    wide,
    a2a_send,
    a2a_recv,
    obs_send,
    obs_recv,
    own_sem,
    go_sem,
    ack_sem,
):
    gx = lax.axis_index("gx")
    gy = lax.axis_index("gy")
    own_members, rows, _ = prior_ref.shape
    members, lanes = spread_ref.shape
    spacing = rows // 2
    height = rows * n_gy
    split = n_gy // 2
    upper = gy >= split
    counts_gx = lax.rem(gx, 2) == 1
    counts_gy = lax.rem(gx, 2) == 0
    partner = gx + 1 - 2 * lax.rem(gx, 2)

    def to_row(step):
        return {"gy": gy + step}

    def peer(step):
        return lax.rem(gx + step, n_gx)

    exists = {step: jnp.logical_and(gy + step >= 0, gy + step < n_gy) for step in OFFSETS}
    crosses = [
        jnp.logical_and(exists[step], jnp.logical_and(upper, gy + step < split)) for step in OFFSETS
    ]
    across = functools.reduce(jnp.logical_or, crosses)
    neighbours = sum(exists[step].astype(jnp.int32) for step in OFFSETS)

    barrier = pltpu.get_barrier_semaphore()
    def greet(chip, carry):
        there = lax.rem(chip + gx // 2, n_gx // 2) * 2 + 1

        @pl.when(there != gx)
        def _():
            pl.semaphore_signal(barrier, inc=1, device_id={"gx": there}, device_id_type=MESH)

        return carry

    for step in OFFSETS:

        @pl.when(exists[step])
        def _():
            pl.semaphore_signal(
                barrier, inc=1, device_id={"gx": gx - lax.rem(gx, 2), "gy": gy + step}, device_id_type=MESH
            )

    @pl.when(counts_gx)
    def _():
        pl.semaphore_signal(barrier, inc=1, device_id={"gx": partner}, device_id_type=MESH)

    lax.fori_loop(0, n_gx // 2, greet, 0)

    own_piece = pltpu.make_async_copy(
        prior_ref.at[:, :, pl.ds(pl.multiple_of(gx * lanes, lanes), lanes)],
        recv.at[pl.ds(gx * own_members, own_members)],
        own_sem.at[0],
    )
    own_obs = pltpu.make_async_copy(
        spread_ref, obs.at[pl.ds(0, members), pl.ds(2 * lanes, lanes)], own_sem.at[1]
    )
    own_misfit = pltpu.make_async_copy(misfit_ref, obs_misfit.at[2], own_sem.at[2])
    own_line = pltpu.make_async_copy(line_ref, obs_line.at[2], own_sem.at[3])
    for copy in (own_piece, own_obs, own_misfit, own_line):
        copy.start()

    def obs_copies(k):
        step = OFFSETS[k]
        slot = 2 - step
        ends = (
            (spread_ref, obs.at[pl.ds(0, members), pl.ds(slot * lanes, lanes)]),
            (misfit_ref, obs_misfit.at[slot]),
            (line_ref, obs_line.at[slot]),
        )
        return [
            pltpu.make_async_remote_copy(
                src_ref=src,
                dst_ref=dst,
                send_sem=obs_send.at[k, j],
                recv_sem=obs_recv.at[k, j],
                device_id=to_row(step),
                device_id_type=MESH,
            )
            for j, (src, dst) in enumerate(ends)
        ]

    sends = [obs_copies(k) for k in range(len(OFFSETS))]

    def piece(step):
        there = peer(step)
        return pltpu.make_async_remote_copy(
            src_ref=prior_ref.at[:, :, pl.ds(pl.multiple_of(there * lanes, lanes), lanes)],
            dst_ref=recv.at[pl.ds(gx * own_members, own_members)],
            send_sem=a2a_send.at[step],
            recv_sem=a2a_recv.at[step],
            device_id={"gx": there},
            device_id_type=MESH,
        )

    def send(t, carry):
        far = n_gx // 2 + ((n_gx - 1 - t) // 2) * (1 - 2 * lax.rem(n_gx - 2 - t, 2))
        piece(far).start()
        return carry

    def start_obs():
        for k, step in enumerate(OFFSETS):

            @pl.when(exists[step])
            def _():
                for copy in sends[k]:
                    copy.start()

    def exchange_gx():
        @pl.when(counts_gx)
        def _():
            pl.semaphore_wait(barrier, n_gx - 1)
            pl.semaphore_signal(go_sem, inc=1, device_id={"gx": partner}, device_id_type=MESH)

        @pl.when(counts_gy)
        def _():
            pl.semaphore_wait(go_sem, 1)

        lax.fori_loop(0, n_gx - 1, send, 0)

    def exchange_gy():
        @pl.when(counts_gy)
        def _():
            pl.semaphore_wait(barrier, 1 + 2 * neighbours)
            pl.semaphore_signal(ack_sem, inc=1, device_id={"gx": partner}, device_id_type=MESH)

        @pl.when(counts_gx)
        def _():
            pl.semaphore_wait(ack_sem, 1)

        start_obs()

    middle = jnp.logical_and(gx // (n_gx // 8) // 2 == 2, jnp.logical_or(gy < split - 2, gy >= split))
    gx_first = jnp.logical_or(across, middle)

    @pl.when(gx_first)
    def _():
        exchange_gx()
        exchange_gy()

    @pl.when(jnp.logical_not(gx_first))
    def _():
        exchange_gy()
        exchange_gx()

    for step in OFFSETS:
        slot = 2 + step

        @pl.when(jnp.logical_not(exists[step]))
        def _():
            obs[:members, slot * lanes : (slot + 1) * lanes] = jnp.zeros((members, lanes), jnp.bfloat16)
            obs_misfit[slot] = jnp.zeros((1, lanes), jnp.bfloat16)
            obs_line[slot] = jnp.zeros((1, lanes), jnp.int32)

    own_obs.wait()
    own_misfit.wait()
    own_line.wait()

    def arrived(k):
        @pl.when(exists[-OFFSETS[k]])
        def _():
            for copy in sends[k]:
                copy.wait_recv()

    def transform(which, first):
        point = 2 * gy + which
        centre = (point.astype(jnp.float32) + 0.5) * spacing
        local = []
        for s in range(first, first + 3):
            tile = gy + s - 2
            position = (tile * rows).astype(jnp.float32) + obs_line[s].astype(jnp.float32) + 0.5
            distance = (position - centre) / float(rows)
            there = jnp.where(jnp.logical_and(tile >= 0, tile < n_gy), 1.0, 0.0)
            local.append(jnp.exp(-0.5 * distance * distance) * there)
        locality = jnp.concatenate(local, axis=1)
        for s in range(first, first + 3):
            obs[members:, s * lanes : (s + 1) * lanes] = jnp.broadcast_to(obs_misfit[s], (16, lanes))
        block = obs[:, first * lanes : (first + 3) * lanes]
        scaled = (block[:members].astype(jnp.float32) * locality).astype(jnp.bfloat16)
        both = mm(block, scaled, NT)
        gram, drive = both[:members], both[members : members + 8]

        n = members - 1.0
        bound = 1.0 + jnp.max(jnp.sum(jnp.abs(gram), axis=0, keepdims=True), axis=1, keepdims=True) / n
        a = 1.0 / bound
        b = a / n
        z0 = 2.25 + a * (-2.4375 + a * (1.6875 + a * (-0.5625 + a * 0.0625)))
        z1 = -2.4375 + a * (3.375 + a * (-1.6875 + a * 0.25))
        z2 = 1.6875 + a * (-1.6875 + a * 0.375)
        z3 = -0.5625 + a * 0.25
        root = lax.rsqrt(bound)
        high = gram.astype(jnp.bfloat16)
        square = mm(high, high)
        inside = square + (z3 * 16.0 / b) * gram
        fourth = mm(square.astype(jnp.bfloat16), inside.astype(jnp.bfloat16))
        b2 = b * b
        t = (root * z1 * b) * gram + (root * z2 * b2) * square + (root * 0.0625 * b2 * b2) * fourth
        th = t.astype(jnp.bfloat16)

        def through(v):
            vh, vl = halves(v)
            both = jnp.concatenate([vh, vl.astype(jnp.bfloat16)], axis=0)
            p = mm(both, th)
            return (p[:8] + p[8:]) * (bound * root) + z0 * v

        weights = through(drive)
        weights = through(weights) / (bound * n)
        return t, weights[:1], z0 * root

    def weight(row, which):
        return hat(gy * rows + row, 2 * gy + which, float(spacing), float(height))

    def mix(row, first, second):
        (p, t, v, d), (p2, t2, v2, d2) = first, second
        wp, wq = weight(row, p), weight(row, p2)
        mixed[row] = (wp * t + wq * t2 + (wp * v + wq * v2)).astype(jnp.bfloat16)
        return wp * d + wq * d2

    arrived(0)
    arrived(1)
    (t0, v0, d0), (t1, v1, d1) = transform(0, 1), transform(1, 1)
    inner[0] = t0
    inner[1] = t1
    k1 = mix(1, (0, t0, v0, d0), (1, t1, v1, d1))
    k2 = mix(2, (0, t0, v0, d0), (1, t1, v1, d1))
    arrived(2)
    arrived(3)
    before, after = transform(-1, 0), transform(2, 2)
    k0 = mix(0, (0, inner[0], v0, d0), (-1, *before))
    k3 = mix(3, (1, inner[1], v1, d1), (2, *after))

    own_piece.wait()

    def land(step, carry):
        piece(step).wait_recv()
        return carry

    lax.fori_loop(1, n_gx, land, 0)

    wide[...] = recv.reshape(members * rows, lanes)[...].astype(jnp.float32)
    for row, diagonal in enumerate((k0, k1, k2, k3)):
        x = wide[pl.ds(row, members, stride=rows), :]
        mean = jnp.sum(x, axis=0, keepdims=True) * (1.0 / members)
        y = mm(mixed[row], (x - mean).astype(jnp.bfloat16))
        x = wide[pl.ds(row, members, stride=rows), :]
        wide[pl.ds(row, members, stride=rows), :] = y + (diagonal * x + (mean - diagonal * mean))
    out_ref[...] = wide[...].astype(jnp.bfloat16)

    def sent(step, carry):
        piece(step).wait_send()
        return carry

    lax.fori_loop(1, n_gx, sent, 0)
    for k, step in enumerate(OFFSETS):

        @pl.when(exists[step])
        def _():
            for copy in sends[k]:
                copy.wait_send()


def solution(mesh):
    n_gx, n_gy = mesh.shape["gx"], mesh.shape["gy"]

    def on_device(prior, spread, misfit, line):
        members, _, lanes = spread.shape
        rows = prior.shape[1]
        out = pl.pallas_call(
            functools.partial(kernel, n_gx, n_gy),
            out_shape=jax.ShapeDtypeStruct((members * rows, lanes), jnp.bfloat16),
            in_specs=[pl.BlockSpec(memory_space=pltpu.HBM)] * 4,
            out_specs=pl.BlockSpec(memory_space=pltpu.VMEM),
            scratch_shapes=[
                pltpu.VMEM((members, rows, lanes), jnp.bfloat16),
                pltpu.VMEM((members + 16, 5 * lanes), jnp.bfloat16),
                pltpu.VMEM((5, 1, lanes), jnp.bfloat16),
                pltpu.VMEM((5, 1, lanes), jnp.int32),
                pltpu.VMEM((2, members, members), jnp.float32),
                pltpu.VMEM((rows, members, members), jnp.bfloat16),
                pltpu.VMEM((members * rows, lanes), jnp.float32),
                pltpu.SemaphoreType.DMA((n_gx,)),
                pltpu.SemaphoreType.DMA((n_gx,)),
                pltpu.SemaphoreType.DMA((4, 3)),
                pltpu.SemaphoreType.DMA((4, 3)),
                pltpu.SemaphoreType.DMA((4,)),
                pltpu.SemaphoreType.REGULAR,
                pltpu.SemaphoreType.REGULAR,
            ],
            compiler_params=pltpu.CompilerParams(
                collective_id=0, has_side_effects=True, vmem_limit_bytes=67043328
            ),
            name="analysis",
        )(prior, spread.reshape(members, lanes), misfit, line)
        return out.reshape(members, rows, lanes)

    return jax.shard_map(
        on_device,
        mesh=mesh,
        in_specs=(P("gx", "gy", None), P(None, "gy", "gx"), P("gy", "gx"), P("gy", "gx")),
        out_specs=P(None, "gy", "gx"),
        check_vma=False,
    )
```

```python
import functools

import jax
import jax.numpy as jnp
from jax import lax
from jax.experimental import pallas as pl
from jax.experimental.pallas import tpu as pltpu
from jax.sharding import PartitionSpec as P

MESH = pl.DeviceIdType.MESH
NT = (((1,), (1,)), ((), ()))
NN = (((1,), (0,)), ((), ()))
OFFSETS = (1, -1, 2, -2)


def mm(a, b, dims=NN):
    return lax.dot_general(a, b, dims, preferred_element_type=jnp.float32)


def halves(x):
    high = x.astype(jnp.bfloat16)
    return high, x - high.astype(jnp.float32)


def hat(row, point, spacing, height):
    r = jnp.clip(row.astype(jnp.float32) + 0.5, 0.5 * spacing, height - 0.5 * spacing)
    centre = (point.astype(jnp.float32) + 0.5) * spacing
    return jnp.maximum(0.0, 1.0 - jnp.abs(r - centre) / spacing)


def kernel(
    n_gx,
    n_gy,
    prior_ref,
    spread_ref,
    misfit_ref,
    line_ref,
    out_ref,
    recv,
    obs,
    obs_misfit,
    obs_line,
    inner,
    mixed,
    wide,
    a2a_send,
    a2a_recv,
    obs_send,
    obs_recv,
    own_sem,
    go_sem,
    ack_sem,
    near_sem,
):
    gx = lax.axis_index("gx")
    gy = lax.axis_index("gy")
    own_members, rows, _ = prior_ref.shape
    members, lanes = spread_ref.shape
    spacing = rows // 2
    height = rows * n_gy
    split = n_gy // 2
    upper = gy >= split

    counts_gx = lax.rem(gx, 2) == 1
    counts_gy = lax.rem(gx, 2) == 0
    partner = gx + 1 - 2 * lax.rem(gx, 2)

    def to_row(step):
        return {"gy": gy + step}

    def peer(step):
        return lax.rem(gx + step, n_gx)

    exists = {step: jnp.logical_and(gy + step >= 0, gy + step < n_gy) for step in OFFSETS}
    crosses = {step: jnp.logical_xor(upper, gy + step >= split) for step in OFFSETS}
    early = {
        step: jnp.logical_and(exists[step], crosses[step] if step > 0 else jnp.logical_not(crosses[step]))
        for step in OFFSETS
    }
    late = {step: jnp.logical_and(exists[step], jnp.logical_not(early[step])) for step in OFFSETS}
    late_near = {step: jnp.logical_and(late[step], jnp.logical_not(crosses[step])) for step in OFFSETS}
    late_across = {step: jnp.logical_and(late[step], crosses[step]) for step in OFFSETS}

    def count(flags):
        return sum(flags[step].astype(jnp.int32) for step in OFFSETS)

    barrier = pltpu.get_barrier_semaphore()
    def greet(chip, carry):
        there = lax.rem(chip + gx // 2, n_gx // 2) * 2 + 1

        @pl.when(there != gx)
        def _():
            pl.semaphore_signal(barrier, inc=1, device_id={"gx": there}, device_id_type=MESH)

        return carry

    for step in OFFSETS:

        @pl.when(late[step])
        def _():
            pl.semaphore_signal(
                barrier, inc=1, device_id={"gx": gx - lax.rem(gx, 2), "gy": gy + step}, device_id_type=MESH
            )

    @pl.when(counts_gx)
    def _():
        pl.semaphore_signal(barrier, inc=1, device_id={"gx": partner}, device_id_type=MESH)

    lax.fori_loop(0, n_gx // 2, greet, 0)

    own_piece = pltpu.make_async_copy(
        prior_ref.at[:, :, pl.ds(pl.multiple_of(gx * lanes, lanes), lanes)],
        recv.at[pl.ds(gx * own_members, own_members)],
        own_sem.at[0],
    )
    own_obs = pltpu.make_async_copy(
        spread_ref, obs.at[pl.ds(0, members), pl.ds(2 * lanes, lanes)], own_sem.at[1]
    )
    own_misfit = pltpu.make_async_copy(misfit_ref, obs_misfit.at[2], own_sem.at[2])
    own_line = pltpu.make_async_copy(line_ref, obs_line.at[2], own_sem.at[3])
    for copy in (own_piece, own_obs, own_misfit, own_line):
        copy.start()

    def obs_copies(k):
        step = OFFSETS[k]
        slot = 2 - step
        ends = (
            (spread_ref, obs.at[pl.ds(0, members), pl.ds(slot * lanes, lanes)]),
            (misfit_ref, obs_misfit.at[slot]),
            (line_ref, obs_line.at[slot]),
        )
        return [
            pltpu.make_async_remote_copy(
                src_ref=src,
                dst_ref=dst,
                send_sem=obs_send.at[k, j],
                recv_sem=obs_recv.at[k, j],
                device_id=to_row(step),
                device_id_type=MESH,
            )
            for j, (src, dst) in enumerate(ends)
        ]

    sends = [obs_copies(k) for k in range(len(OFFSETS))]

    def piece(step):
        there = peer(step)
        return pltpu.make_async_remote_copy(
            src_ref=prior_ref.at[:, :, pl.ds(pl.multiple_of(there * lanes, lanes), lanes)],
            dst_ref=recv.at[pl.ds(gx * own_members, own_members)],
            send_sem=a2a_send.at[step],
            recv_sem=a2a_recv.at[step],
            device_id={"gx": there},
            device_id_type=MESH,
        )

    def send(t, carry):
        place = t // 4
        row = lax.rem(((place + 1) // 2) * (2 * lax.rem(place, 2) - 1) + n_gx, n_gx // 4)
        row = jnp.where(place == 5, 4, jnp.where(place == 6, 3, jnp.where(place == 7, 5, row)))
        there = row * 4 + lax.rem(t + gx, 4)
        step = lax.rem(there - gx + n_gx, n_gx)

        @pl.when(step != 0)
        def _():
            piece(step).start()

        return carry

    def start_obs(flags):
        for k, step in enumerate(OFFSETS):

            @pl.when(flags[step])
            def _():
                for copy in sends[k]:
                    copy.start()

    def exchange_gx():
        @pl.when(counts_gx)
        def _():
            pl.semaphore_wait(barrier, n_gx - 1)
            pl.semaphore_signal(go_sem, inc=1, device_id={"gx": partner}, device_id_type=MESH)

        @pl.when(counts_gy)
        def _():
            pl.semaphore_wait(go_sem, 1)

        lax.fori_loop(0, n_gx, send, 0)

    def say_here(step, core):
        pl.semaphore_signal(
            near_sem.at[crosses[step].astype(jnp.int32)],
            inc=1,
            device_id={"gx": gx - lax.rem(gx, 2) + core, "gy": gy + step},
            device_id_type=MESH,
        )

    @pl.when(counts_gy)
    def _():
        pl.semaphore_wait(barrier, 1 + 2 * count(early))
        pl.semaphore_signal(ack_sem, inc=1, device_id={"gx": partner}, device_id_type=MESH)
        for step in OFFSETS:

            @pl.when(early[step])
            def _():
                say_here(step, 0)
                say_here(step, 1)

    @pl.when(counts_gx)
    def _():
        pl.semaphore_wait(ack_sem, 1)

    second = {step: jnp.logical_and(early[step], gy == split - 2) if step == 2 else False for step in OFFSETS}
    start_obs({step: jnp.logical_and(early[step], jnp.logical_not(second[step])) for step in OFFSETS})

    middle = jnp.logical_and(gx // (n_gx // 8) // 2 == 2, jnp.logical_or(gy < split - 2, upper))

    @pl.when(middle)
    def _():
        exchange_gx()

    @pl.when(count(late_near) > 0)
    def _():
        pl.semaphore_wait(near_sem.at[0], count(late_near))

    start_obs({step: jnp.logical_or(late_near[step], second[step]) for step in OFFSETS})

    @pl.when(jnp.logical_not(middle))
    def _():
        exchange_gx()

    @pl.when(count(late_across) > 0)
    def _():
        pl.semaphore_wait(near_sem.at[1], count(late_across))
        start_obs(late_across)

    for step in OFFSETS:
        slot = 2 + step

        @pl.when(jnp.logical_not(exists[step]))
        def _():
            obs[:members, slot * lanes : (slot + 1) * lanes] = jnp.zeros((members, lanes), jnp.bfloat16)
            obs_misfit[slot] = jnp.zeros((1, lanes), jnp.bfloat16)
            obs_line[slot] = jnp.zeros((1, lanes), jnp.int32)

    own_obs.wait()
    own_misfit.wait()
    own_line.wait()

    def arrived(k):
        @pl.when(exists[-OFFSETS[k]])
        def _():
            for copy in sends[k]:
                copy.wait_recv()

    def transform(which, first):
        point = 2 * gy + which
        centre = (point.astype(jnp.float32) + 0.5) * spacing
        local = []
        for s in range(first, first + 3):
            tile = gy + s - 2
            position = (tile * rows).astype(jnp.float32) + obs_line[s].astype(jnp.float32) + 0.5
            distance = (position - centre) / float(rows)
            there = jnp.where(jnp.logical_and(tile >= 0, tile < n_gy), 1.0, 0.0)
            local.append(jnp.exp(-0.5 * distance * distance) * there)
        locality = jnp.concatenate(local, axis=1)
        for s in range(first, first + 3):
            obs[members:, s * lanes : (s + 1) * lanes] = jnp.broadcast_to(obs_misfit[s], (16, lanes))
        block = obs[:, first * lanes : (first + 3) * lanes]
        scaled = (block[:members].astype(jnp.float32) * locality).astype(jnp.bfloat16)
        both = mm(block, scaled, NT)
        gram, drive = both[:members], both[members : members + 8]

        n = members - 1.0
        bound = 1.0 + jnp.max(jnp.sum(jnp.abs(gram), axis=0, keepdims=True), axis=1, keepdims=True) / n
        a = 1.0 / bound
        b = a / n
        z0 = 2.25 + a * (-2.4375 + a * (1.6875 + a * (-0.5625 + a * 0.0625)))
        z1 = -2.4375 + a * (3.375 + a * (-1.6875 + a * 0.25))
        z2 = 1.6875 + a * (-1.6875 + a * 0.375)
        z3 = -0.5625 + a * 0.25
        root = lax.rsqrt(bound)
        high = gram.astype(jnp.bfloat16)
        square = mm(high, high)
        inside = square + (z3 * 16.0 / b) * gram
        fourth = mm(square.astype(jnp.bfloat16), inside.astype(jnp.bfloat16))
        b2 = b * b
        t = (root * z1 * b) * gram + (root * z2 * b2) * square + (root * 0.0625 * b2 * b2) * fourth
        th = t.astype(jnp.bfloat16)

        def through(v):
            vh, vl = halves(v)
            both = jnp.concatenate([vh, vl.astype(jnp.bfloat16)], axis=0)
            p = mm(both, th)
            return (p[:8] + p[8:]) * (bound * root) + z0 * v

        weights = through(drive)
        weights = through(weights) / (bound * n)
        return t, weights[:1], z0 * root

    def weight(row, which):
        return hat(gy * rows + row, 2 * gy + which, float(spacing), float(height))

    def mix(row, first, second):
        (p, t, v, d), (p2, t2, v2, d2) = first, second
        wp, wq = weight(row, p), weight(row, p2)
        mixed[row] = (wp * t + wq * t2 + (wp * v + wq * v2)).astype(jnp.bfloat16)
        return wp * d + wq * d2

    arrived(0)
    arrived(1)
    (t0, v0, d0), (t1, v1, d1) = transform(0, 1), transform(1, 1)
    inner[0] = t0
    inner[1] = t1
    k1 = mix(1, (0, t0, v0, d0), (1, t1, v1, d1))
    k2 = mix(2, (0, t0, v0, d0), (1, t1, v1, d1))
    arrived(2)
    arrived(3)
    before, after = transform(-1, 0), transform(2, 2)
    k0 = mix(0, (0, inner[0], v0, d0), (-1, *before))
    k3 = mix(3, (1, inner[1], v1, d1), (2, *after))

    def sent(step, carry):
        piece(step).wait_send()
        return carry

    lax.fori_loop(1, n_gx, sent, 0)
    for k, step in enumerate(OFFSETS):

        @pl.when(exists[step])
        def _():
            for copy in sends[k]:
                copy.wait_send()

    own_piece.wait()

    def land(step, carry):
        piece(step).wait_recv()
        return carry

    lax.fori_loop(1, n_gx, land, 0)

    wide[...] = recv.reshape(members * rows, lanes)[...].astype(jnp.float32)
    for row, diagonal in enumerate((k0, k1, k2, k3)):
        x = wide[pl.ds(row, members, stride=rows), :]
        mean = jnp.sum(x, axis=0, keepdims=True) * (1.0 / members)
        y = mm(mixed[row], (x - mean).astype(jnp.bfloat16))
        x = wide[pl.ds(row, members, stride=rows), :]
        wide[pl.ds(row, members, stride=rows), :] = y + (diagonal * x + (mean - diagonal * mean))
    out_ref[...] = wide[...].astype(jnp.bfloat16)


def solution(mesh):
    n_gx, n_gy = mesh.shape["gx"], mesh.shape["gy"]

    def on_device(prior, spread, misfit, line):
        members, _, lanes = spread.shape
        rows = prior.shape[1]
        out = pl.pallas_call(
            functools.partial(kernel, n_gx, n_gy),
            out_shape=jax.ShapeDtypeStruct((members * rows, lanes), jnp.bfloat16),
            in_specs=[pl.BlockSpec(memory_space=pltpu.HBM)] * 4,
            out_specs=pl.BlockSpec(memory_space=pltpu.VMEM),
            scratch_shapes=[
                pltpu.VMEM((members, rows, lanes), jnp.bfloat16),
                pltpu.VMEM((members + 16, 5 * lanes), jnp.bfloat16),
                pltpu.VMEM((5, 1, lanes), jnp.bfloat16),
                pltpu.VMEM((5, 1, lanes), jnp.int32),
                pltpu.VMEM((2, members, members), jnp.float32),
                pltpu.VMEM((rows, members, members), jnp.bfloat16),
                pltpu.VMEM((members * rows, lanes), jnp.float32),
                pltpu.SemaphoreType.DMA((n_gx,)),
                pltpu.SemaphoreType.DMA((n_gx,)),
                pltpu.SemaphoreType.DMA((4, 3)),
                pltpu.SemaphoreType.DMA((4, 3)),
                pltpu.SemaphoreType.DMA((4,)),
                pltpu.SemaphoreType.REGULAR,
                pltpu.SemaphoreType.REGULAR,
                pltpu.SemaphoreType.REGULAR((2,)),
            ],
            compiler_params=pltpu.CompilerParams(
                collective_id=0, has_side_effects=True, vmem_limit_bytes=67043328
            ),
            name="analysis",
        )(prior, spread.reshape(members, lanes), misfit, line)
        return out.reshape(members, rows, lanes)

    return jax.shard_map(
        on_device,
        mesh=mesh,
        in_specs=(P("gx", "gy", None), P(None, "gy", "gx"), P("gy", "gx"), P("gy", "gx")),
        out_specs=P(None, "gy", "gx"),
        check_vma=False,
    )
```
